32 devices in a mesh: occ: 8 (over z, x), rep: 4 (over y, core).
Axes of the slice: x: 2, y: 2, z: 4, core: 2. Of those that a mesh axis runs over, the one named last changes fastest.
Arguments:
- coeffs: bfloat16 [128, 12, 64, 128], P(('occ', 'rep')), may hold values from -1 to 1
- amplitudes: bfloat16 [128, 4096], P(('occ', 'rep')), may hold values from -6 to 6
- denominators: float32 [128, 64], P(('occ', 'rep')), may hold values from 0.25 to 2
- pno_count: int32 [128], P(('occ', 'rep')), may hold values from 24 to 64
- domains: int32 [128, 12], replicated, may hold values from 0 to 31, as said below
- far_owner: int32 [128, 2], P(('occ', 'rep')), may hold values from 0 to 7, all different within a row; in each aligned block of 4 rows (0 to 3, 4 to 7, ...) at most 2 rows name the same one
- far_pair: int32 [128, 2], P(('occ', 'rep')), may hold values from 0 to 3
- near_pair: int32 [128, 40], P(('occ', 'rep')), may hold values from 0 to 15
Outputs:
- residual: float32 [128, 4096], P(('occ', 'rep'))
The draws below stay inside these ranges and needn't reach their ends.
Inputs may be any that keep to these rules, and one draw needn't show every extreme that they name: `domains`: each row names 12 different blocks. `far_owner`: the 2 entries of a row differ; among the rows of one device no occupied block is named more than 2 times, and that bound is reached.
All inputs are finite; a program needn't handle non-finite values.
Results may differ from the reference program's by a relative error of at most 0.0003.
Values may be sent and summed in bfloat16 or wider, within the bound.
No kernel may reach another device: no remote copies, remote signals or barrier semaphores. Data moves between devices by JAX's collectives and lax.ppermute only.
A program may use at most 128 MiB of HBM per device.

```python
import math
import jax
import jax.numpy as jnp
import numpy as np
from jax import lax

NPNO = 64
BLK = 128
DOMB = 12
NBLK = 32
KN = 2
KL = 40
P_DEV = 4
NP = 128
CAP = 2
N_OCC = 8
N_REP = 4


def draw_domains(key, part):
    row_keys = jax.random.split(jax.random.fold_in(key, 7), NP)
    picked = jax.vmap(lambda row_key: jax.random.permutation(row_key, NBLK)[:DOMB])(row_keys)
    return picked.astype(jnp.int32)


def place_ends(entries, key, smallest, top_value):
    shape = entries.shape
    index_at = [jax.random.randint(jax.random.fold_in(key, axis), (), 0, shape[axis]) for axis in range(len(shape))]
    entries = entries.at[tuple(index_at)].set(smallest)
    longest = shape.index(max(shape))
    index_at[longest] = (index_at[longest] + 1) % shape[longest]
    return entries.at[tuple(index_at)].set(top_value)


def block_levels(own_key, extent, shards, low, largest):
    factor_of = 1.0
    for axis_at, shards_of in shards:
        steps = jax.random.uniform(jax.random.fold_in(jax.random.fold_in(own_key, 6), axis_at), (shards_of,), jnp.float32, low / len(shards), largest / len(shards))
        factor_of = factor_of * jnp.repeat(jnp.exp(steps), extent[axis_at] // shards_of).reshape((-1,) + (1,) * (len(extent) - 1 - axis_at))
    return factor_of


def deal_out(own_key, own, number, rows, count, top, most, skew):
    sequence = jax.random.permutation(own_key, count)
    packed, common = shares(count, rows * top, most, skew, True), shares(count, rows * top, most, skew, False)
    places = jnp.arange(count)

    def named(lengths, rotation):
        used = int((lengths > 0).sum())
        fixed = max(1, used // 4)
        shifted = fixed + (places - fixed + rotation * (used - fixed)) % max(1, count - fixed)
        return jnp.zeros((count,), jnp.int32).at[sequence[jnp.where(places < fixed, places, shifted)]].set(jnp.asarray(lengths, jnp.int32))

    lengths = jnp.where(number % 4 == 0, named(packed, number // 4), named(common, number - number // 4 - 1))
    mixed = jax.random.permutation(jax.random.fold_in(own, 3), count)
    source_of, sink = mixed[0:count // 2 * 2:2], mixed[1:count // 2 * 2:2]
    slack = jnp.minimum(lengths[source_of] - 1, most - lengths[sink]) // 2
    slack = jnp.where((source_of == sequence[0]) | (sink == sequence[0]) | (lengths[sink] == 0), 0, jnp.maximum(slack, 0))
    shifted = jax.random.randint(jax.random.fold_in(own, 4), (count // 2,), 0, 1 << 20) % (slack + 1)
    lengths = lengths.at[source_of].add(-shifted).at[sink].add(shifted)
    members = jnp.searchsorted(jnp.cumsum(lengths), jnp.arange(rows * top), side="right").astype(jnp.int32)
    grid = members.reshape(top, rows).T
    grid = grid[jax.random.permutation(jax.random.fold_in(own, 1), rows)]
    rotation = jax.random.randint(jax.random.fold_in(own, 2), (rows, 1), 0, top)
    return jnp.take_along_axis(grid, (jnp.arange(top)[None, :] + rotation) % top, axis=1)


def shares(amount, total, limit, skew, full):
    weights = [(1 << 20) // math.isqrt(standing ** skew) + 1 for standing in range(1, amount + 1)]
    largest = limit if full else min(limit, max(-(-total // amount), total * weights[0] // sum(weights)))
    least = 1 if total - largest >= amount - 1 else 0
    holding, surplus = [largest] + [least] * (amount - 1), total - largest - least * (amount - 1)
    while surplus > 0:
        free = [i for i in range(1, amount) if holding[i] < largest] or [i for i in range(1, amount) if holding[i] < limit]
        whole, remaining = sum([weights[i] for i in free]), surplus
        for i in free:
            extra = min(limit - holding[i], max(1, remaining * weights[i] // whole), surplus)
            holding[i] = holding[i] + extra
            surplus = surplus - extra
    return np.array(holding)


def gaussian(key, extent, spread, most, shards=(), held_as=jnp.bfloat16):
    values = spread * jax.random.normal(key, extent, jnp.float32)
    if shards:
        values = values * block_levels(key, extent, shards, -0.22, 0.18)
    return jnp.clip(values, -most, most).astype(held_as)


def setup_inputs(seed: int = 0) -> dict:
    seeds = jax.random.split(jax.random.key(seed), 9)
    coeffs = gaussian(seeds[0], (NP, DOMB, NPNO, BLK), ((NPNO * DOMB * DOMB * BLK / NBLK) ** -0.25), 1.0, ((0, 32),))
    amplitudes = gaussian(seeds[1], (NP, NPNO * NPNO), 1.0, 6.0, ((0, 32),))
    denominators = jnp.clip(jnp.exp(math.log(2.0) - 2.0794415 * jax.random.uniform(seeds[2], (NP, NPNO), jnp.float32) ** block_levels(seeds[2], (NP, NPNO), ((0, 32),), -0.2, 0.2)), 0.25, 2.0)
    pno_count = place_ends(jax.random.randint(seeds[3], (NP,), 3 * NPNO // 8, NPNO + 1), jax.random.fold_in(seeds[3], 1), 3 * NPNO // 8, NPNO).astype(jnp.int32)
    domains = draw_domains(jax.random.fold_in(seeds[8], 71), 0)
    far_owner_keys = jax.random.split(jax.random.fold_in(seeds[5], 1), NP // P_DEV)
    far_owner_turns = jax.random.permutation(jax.random.fold_in(seeds[5], 3), NP // P_DEV)
    far_owner = jax.vmap(lambda own, number: deal_out(jax.random.fold_in(seeds[5], 2), own, number, P_DEV, N_OCC, KN, CAP, 2))(far_owner_keys, far_owner_turns).reshape((NP, KN))
    far_pair = place_ends(jax.random.randint(seeds[6], (NP, KN), 0, P_DEV), jax.random.fold_in(seeds[6], 1), 0, P_DEV - 1).astype(jnp.int32)
    near_pair = place_ends(jax.random.randint(seeds[7], (NP, KL), 0, N_REP * P_DEV), jax.random.fold_in(seeds[7], 1), 0, (N_REP * P_DEV) - 1).astype(jnp.int32)
    return dict(coeffs=coeffs, amplitudes=amplitudes, denominators=denominators, pno_count=pno_count, domains=domains, far_owner=far_owner, far_pair=far_pair, near_pair=near_pair)


def intersection(left_coeff, left_dom, right_coeff, right_dom):
    matches = (left_dom[:, None] == right_dom[None, :]).astype(jnp.float32)
    flat = right_coeff.reshape(right_coeff.shape[0], -1).astype(jnp.float32)
    aligned = jnp.dot(matches, flat, precision=lax.Precision.HIGHEST).reshape(right_coeff.shape)
    per_block = jnp.einsum('arc,asc->ars', left_coeff.astype(jnp.float32), aligned, precision=lax.Precision.HIGHEST)
    return jnp.sum(per_block, axis=0)


def reference(coeffs, amplitudes, denominators, pno_count, domains, far_owner, far_pair, near_pair):
    pair_total = coeffs.shape[0]
    live_rows = jnp.arange(NPNO, dtype=jnp.int32)[None, :] < pno_count[:, None]
    live_both = live_rows[:, :, None] & live_rows[:, None, :]
    amp_square = amplitudes.reshape(pair_total, NPNO, NPNO).astype(jnp.float32)
    amp_masked = jnp.where(live_both, amp_square, jnp.zeros((), jnp.float32))
    pair_ids = jnp.arange(pair_total, dtype=jnp.int32)
    device = pair_ids // P_DEV
    owner_occ = device // N_REP
    owner_rep = device % N_REP
    near_ids = (owner_occ[:, None] * (N_REP * P_DEV) + near_pair).astype(jnp.int32)
    far_ids = ((far_owner * N_REP + owner_rep[:, None]) * P_DEV + far_pair).astype(jnp.int32)
    all_ids = jnp.concatenate([near_ids, far_ids], axis=1)

    def masked_coeff(index):
        return jnp.where(live_rows[index][..., None, :, None], coeffs[index], jnp.zeros((), coeffs.dtype))

    def pair_terms(pair_index):
        others = all_ids[pair_index]
        left_coeff = masked_coeff(pair_index)
        intersections = jax.vmap(intersection, in_axes=(None, None, 0, 0))(left_coeff, domains[pair_index], masked_coeff(others), domains[others])
        gain_terms = jnp.einsum('kab,kbc,kdc->ad', intersections, amp_masked[others], intersections, precision=lax.Precision.HIGHEST)
        far_over = intersections[KL:]
        back_terms = jnp.einsum('kba,bc,kcd->kad', far_over, amp_masked[pair_index], far_over, precision=lax.Precision.HIGHEST)
        return gain_terms, back_terms

    gain_terms, back_terms = lax.map(pair_terms, pair_ids)
    back_sum = jax.ops.segment_sum(back_terms.reshape(pair_total * KN, NPNO, NPNO), far_ids.reshape(-1), pair_total)
    denominator_sum = denominators[:, :, None] + denominators[:, None, :]
    residual = denominator_sum * amp_masked + gain_terms + back_sum
    residual = jnp.where(live_both, residual, jnp.zeros((), jnp.float32))
    return residual.reshape(pair_total, NPNO * NPNO)
```

```python
import functools

import jax
import jax.numpy as jnp
from jax import lax
from jax.experimental import pallas as pl
from jax.experimental.pallas import tpu as pltpu
from jax.sharding import PartitionSpec as P

NPNO = 64
NBLK = 32
ABSENT = 1 << 20
NOBODY = -(1 << 16)
EXT_ROWS = NPNO + 8
F32 = jnp.float32
BF16 = jnp.bfloat16
NT = (((1,), (1,)), ((), ()))
TN = (((0,), (0,)), ((), ()))


def split(value):
    high = value.astype(BF16)
    return high, (value - high.astype(F32)).astype(BF16)


def contract_kernel(p_slots, q_slots, near_rows, silent, pairs, blocks, meta, inv, near, *refs):
    count = (len(refs) - 9) // 2
    units, exts = refs[:count], refs[count : 2 * count]
    out, pool, dense, x_hi, x_lo, v_hi, v_lo, diag, sems = refs[2 * count :]
    per_unit = pairs * blocks
    rows = pairs * NPNO
    zero_at = count * per_unit
    copies = [
        pltpu.make_async_copy(units[u], pool.at[pl.ds(u * per_unit, per_unit)], sems.at[u])
        for u in range(count)
    ]
    for copy in copies:
        copy.start()
    pool[zero_at] = jnp.zeros(pool.shape[1:], BF16)
    diag[...] = jnp.zeros(diag.shape, BF16)
    waited = set()

    def arrive(u):
        if u not in waited:
            waited.add(u)
            copies[u].wait()

    def block_of(u, j, d):
        at = inv[(meta[1, u] + j) * NBLK + d] + (u * per_unit + j * blocks)
        return pool[jnp.minimum(at, zero_at)]

    for i, u in enumerate(p_slots):
        arrive(u)
        for j in range(pairs):
            for d in range(NBLK):
                dense[pl.ds(i * rows + j * NPNO, NPNO), pl.ds(d * 128, 128)] = block_of(u, j, d)

    lane = lax.broadcasted_iota(jnp.int32, (1, rows), 1)
    pair_of_lane = (lane // NPNO).astype(F32)
    left = lax.broadcasted_iota(jnp.int32, (NPNO, 128), 1) < NPNO
    for i, u in enumerate(q_slots):
        arrive(u)
        lhs = jnp.concatenate(
            [
                jnp.concatenate([block_of(u, j, d) for d in range(NBLK)], axis=1)
                for j in range(pairs)
            ],
            axis=0,
        )
        x = lax.dot_general(lhs, dense[...], NT, preferred_element_type=F32)
        xh, xl = split(x)
        here = pl.ds(i * rows, rows)
        x_hi[here, :] = xh
        x_lo[here, :] = xl
        for j in range(pairs):
            tile = exts[u][j // 2, :NPNO, :]
            keep = left if j % 2 == 0 else jnp.logical_not(left)
            diag[pl.ds(j * NPNO, NPNO), pl.ds((j // 2) * 128, 128)] = jnp.where(
                keep, tile.astype(F32), 0.0
            ).astype(BF16)
        amps = diag[...]
        v = jnp.dot(amps, xh, preferred_element_type=F32) + jnp.dot(
            amps, xl, preferred_element_type=F32
        )
        parts = []
        for n, s in enumerate(p_slots):
            p_id = meta[0, s].astype(F32) + pair_of_lane
            tails = [exts[s][h, NPNO:, :].astype(F32) for h in range(pairs // 2)]
            p_codes = [jnp.concatenate([t[k : k + 1] for t in tails], axis=1) for k in range(2)]
            strips = []
            for j in range(pairs):
                weight = jnp.zeros((1, rows), F32)
                if (u, s) not in silent:
                    q_id = (meta[0, u] + j).astype(F32)
                    q_tail = exts[u][j // 2, NPNO:, :].astype(F32)
                    for k in range(2):
                        at = 2 + 2 * (j % 2) + k
                        q_code = jnp.concatenate([q_tail[at : at + 1]] * (pairs // 2), axis=1)
                        weight = weight + jnp.where(q_code == p_id, 1.0, 0.0)
                        weight = weight + jnp.where(p_codes[k] == q_id, 1.0, 0.0)
                if n == 0 and u in near_rows:
                    at = near_rows[u] + j
                    weight = weight + near[at : at + 1, :]
                strips.append(
                    v[j * NPNO : (j + 1) * NPNO, n * rows : (n + 1) * rows] * weight
                )
            parts.append(jnp.concatenate(strips, axis=0))
        v = jnp.concatenate(parts, axis=1) if len(parts) > 1 else parts[0]
        vh, vl = split(v)
        v_hi[here, :] = vh
        v_lo[here, :] = vl

    row = lax.broadcasted_iota(jnp.int32, (rows, rows), 0) // NPNO
    col = lax.broadcasted_iota(jnp.int32, (rows, rows), 1) // NPNO
    own_block = row == col
    for i in range(len(p_slots)):
        cols = pl.ds(i * rows, rows)
        xh, xl, vh, vl = x_hi[:, cols], x_lo[:, cols], v_hi[:, cols], v_lo[:, cols]
        total = lax.dot_general(xh, vh, TN, preferred_element_type=F32)
        total += lax.dot_general(xh, vl, TN, preferred_element_type=F32)
        total += lax.dot_general(xl, vh, TN, preferred_element_type=F32)
        total = jnp.where(own_block, total, 0.0)
        for h in range(pairs // 2):
            two = total[h * 128 : (h + 1) * 128, h * 128 : (h + 1) * 128]
            out[i, h] = two[:NPNO] + two[NPNO:]


def contract(units, exts, meta, inv, near, p_slots, q_slots, near_rows=None, silent=()):
    near_rows = near_rows or {}
    count = len(units)
    pairs = exts[0].shape[0] * 2
    blocks = units[0].shape[0] // pairs
    rows = pairs * NPNO
    p_rows, q_rows = len(p_slots) * rows, len(q_slots) * rows
    smem = pl.BlockSpec(memory_space=pltpu.SMEM)
    vmem = pl.BlockSpec(memory_space=pltpu.VMEM)
    anywhere = pl.BlockSpec(memory_space=pl.ANY)
    body = functools.partial(
        contract_kernel, p_slots, q_slots, near_rows, frozenset(silent), pairs, blocks
    )
    flops = 2 * p_rows * q_rows * (NBLK * 128 + 5 * rows)
    return pl.pallas_call(
        body,
        out_shape=jax.ShapeDtypeStruct((len(p_slots), pairs // 2, NPNO, 128), F32),
        in_specs=[smem, smem, vmem] + [anywhere] * count + [vmem] * count,
        out_specs=vmem,
        scratch_shapes=[
            pltpu.VMEM((count * pairs * blocks + 1, NPNO, 128), BF16),
            pltpu.VMEM((p_rows, NBLK * 128), BF16),
            pltpu.VMEM((q_rows, p_rows), BF16),
            pltpu.VMEM((q_rows, p_rows), BF16),
            pltpu.VMEM((q_rows, p_rows), BF16),
            pltpu.VMEM((q_rows, p_rows), BF16),
            pltpu.VMEM((rows, rows), BF16),
            pltpu.SemaphoreType.DMA((count,)),
        ],
        cost_estimate=pl.CostEstimate(flops=flops, bytes_accessed=0, transcendentals=0),
        compiler_params=pltpu.CompilerParams(vmem_limit_bytes=48 << 20),
    )(meta, inv, near, *units, *exts)


def pack(square):
    pairs = square.shape[0]
    return (
        square.reshape(pairs // 2, 2, NPNO, NPNO).transpose(0, 2, 1, 3).reshape(pairs // 2, NPNO, 128)
    )


def unpack(packed):
    halves = packed.shape[0]
    return packed.reshape(halves, NPNO, 2, NPNO).transpose(0, 2, 1, 3).reshape(2 * halves, NPNO * NPNO)


def on_device(coeffs, amplitudes, denominators, pno_count, domains, far_owner, far_pair, near_pair):
    pairs, blocks = coeffs.shape[:2]
    occ_count = lax.axis_size("occ")
    rep_count = lax.axis_size("rep")
    occ = lax.axis_index("occ")
    rep = lax.axis_index("rep")
    live_rows = jnp.arange(NPNO, dtype=jnp.int32)[None, :] < pno_count[:, None]
    live_both = live_rows[:, :, None] & live_rows[:, None, :]
    amps = jnp.where(
        live_both, amplitudes.reshape(pairs, NPNO, NPNO), jnp.zeros((), BF16)
    )
    codes = (far_owner * pairs + far_pair + 1).astype(BF16).reshape(pairs // 2, 2, 2)
    ext = jnp.concatenate(
        [
            pack(amps),
            jnp.broadcast_to(
                codes.transpose(0, 2, 1)[..., None], (pairs // 2, 2, 2, NPNO)
            ).reshape(pairs // 2, 2, 128),
            jnp.broadcast_to(codes.reshape(pairs // 2, 4, 1), (pairs // 2, 4, 128)),
            jnp.zeros((pairs // 2, 2, 128), BF16),
        ],
        axis=1,
    )
    block_ids = jnp.arange(NBLK, dtype=jnp.int32)
    inv = jnp.min(
        jnp.where(
            domains[:, None, :] == block_ids[None, :, None],
            jnp.arange(blocks, dtype=jnp.int32)[None, None, :],
            ABSENT,
        ),
        axis=2,
    ).reshape(-1)
    own = coeffs.reshape(pairs * blocks, NPNO, 128)
    group_index = jnp.arange(rep_count * pairs, dtype=jnp.int32)
    slot_pair = ((group_index // pairs) ^ rep) * pairs + group_index % pairs
    near_weight = jnp.sum(
        (near_pair[None, :, :] == slot_pair[:, None, None]).astype(F32), axis=2
    )
    near = jnp.repeat(near_weight, NPNO, axis=1)
    base = pack(
        (denominators[:, :, None] + denominators[:, None, :]) * amps.astype(F32)
    )
    mask = pack(live_both.astype(F32))

    def pair_base(o, r):
        return (o * rep_count + r) * pairs

    def table(ids, bases):
        return jnp.stack([jnp.stack(ids), jnp.stack(bases)]).astype(jnp.int32)

    nobody = jnp.full((), NOBODY, jnp.int32)
    near_reps = [rep ^ k for k in range(rep_count)]

    if occ_count == 8 and rep_count == 4:
        layer, side = occ // 2, occ % 2
        inner = (layer == 1) | (layer == 2)
        end = jnp.where(layer < 2, 0, 3)
        occ_ids = [
            occ,
            end * 2 + side,
            (3 - layer) * 2 + side,
            layer * 2 + 1 - side,
            (3 - end) * 2 + side,
            end * 2 + 1 - side,
        ]
        ids = [occ * pairs + 1] + [
            jnp.where(inner, o * pairs + 1, nobody) for o in occ_ids[1:]
        ]
        bases = [pair_base(o, rep) for o in occ_ids]
        to_inner = [(s, 2 + s) for s in range(2)] + [(6 + s, 4 + s) for s in range(2)]
        from_inner = [(b, a) for a, b in to_inner]
        middle = [(a, a ^ 6) for a in range(2, 6)]
        across = [(a, a ^ 1) for a in range(2, 6)]
        swap_y = [(r, r ^ 2) for r in range(rep_count)]
        swap_core = [(r, r ^ 1) for r in range(rep_count)]
        both = (own, ext)

        def send(values, axis, perm):
            return tuple(lax.ppermute(v, axis, perm) for v in values)

        outer = send(both, "occ", to_inner)
        mid1 = send(both, "occ", middle)
        side1 = send(both, "occ", across)
        other_y = send(both, "rep", swap_y)
        other_core = send(both, "rep", swap_core)
        mid2 = send(outer, "occ", middle)
        side2 = send(outer, "occ", across)
        other_both = send(other_y, "rep", swap_core)

        def units_of(*items):
            return [u for u, _ in items], [e for _, e in items]

        first = contract(
            *units_of(both, outer, mid1, side1),
            table(ids[:4], bases[:4]),
            inv,
            near,
            (0, 1),
            (0, 1, 2, 3),
            near_rows={0: 0},
            silent=((1, 1),),
        )
        close = contract(
            *units_of(both, other_core, other_y, other_both),
            table([nobody] * 4, [pair_base(occ, r) for r in near_reps]),
            inv,
            near,
            (0,),
            (1, 2, 3),
            near_rows={k: k * pairs for k in range(1, 4)},
            silent=((1, 0), (2, 0), (3, 0)),
        )
        crossed = contract(
            *units_of(side1, side2, mid1, mid2),
            table([ids[3], ids[5], ids[2], ids[4]], [bases[3], bases[5], bases[2], bases[4]]),
            inv,
            near,
            (0, 1),
            (2, 3),
        )
        returned = lax.ppermute(crossed, "occ", across)
        last = contract(
            *units_of(both, outer, mid2, side2),
            table([ids[0], ids[1], ids[4], ids[5]], [bases[0], bases[1], bases[4], bases[5]]),
            inv,
            near,
            (0, 1),
            (2, 3),
        )
        total = first + last + returned
        home = lax.ppermute(total[1], "occ", from_inner)
        gain = total[0] + close[0] + home
    else:
        group_units = lax.all_gather(own, "rep", axis=0)
        group_exts = lax.all_gather(ext, "rep", axis=0)
        line_units = lax.all_gather(own, "occ", axis=0)
        line_exts = lax.all_gather(ext, "occ", axis=0)

        def add_near(total, k):
            r = rep ^ k
            rows = lax.dynamic_slice_in_dim(near, k * pairs, pairs, 0)
            part = contract(
                [own, group_units[r]],
                [ext, group_exts[r]],
                table([nobody, nobody], [pair_base(occ, rep), pair_base(occ, r)]),
                inv,
                rows,
                (0,),
                (1,),
                near_rows={1: 0},
                silent=((1, 0),),
            )
            return total + part[0], None

        def add_far(total, o):
            part = contract(
                [own, line_units[o]],
                [ext, line_exts[o]],
                table(
                    [occ * pairs + 1, o * pairs + 1], [pair_base(occ, rep), pair_base(o, rep)]
                ),
                inv,
                near,
                (0,),
                (1,),
            )
            return total + part[0], None

        gain = jnp.zeros(base.shape, F32)
        gain, _ = lax.scan(add_near, gain, jnp.arange(rep_count, dtype=jnp.int32))
        gain, _ = lax.scan(add_far, gain, jnp.arange(occ_count, dtype=jnp.int32))
    return unpack(jnp.where(mask > 0, base + gain, 0.0))


def solution(mesh):
    in_specs = (
        P(("occ", "rep"), None, None, None),
        P(("occ", "rep"), None),
        P(("occ", "rep"), None),
        P(("occ", "rep")),
        P(),
        P(("occ", "rep"), None),
        P(("occ", "rep"), None),
        P(("occ", "rep"), None),
    )
    out_specs = P(("occ", "rep"), None)
    return jax.shard_map(
        on_device, mesh=mesh, in_specs=in_specs, out_specs=out_specs, check_vma=False
    )
```

```python
import functools

import jax
import jax.numpy as jnp
from jax import lax
from jax.experimental import pallas as pl
from jax.experimental.pallas import tpu as pltpu
from jax.sharding import PartitionSpec as P


NPNO = 64
NBLK = 32
ABSENT = 1 << 10
GRANT = 16 << 20
NOBODY = -(1 << 16)
F32 = jnp.float32
BF16 = jnp.bfloat16
NT = (((1,), (1,)), ((), ()))
TN = (((0,), (0,)), ((), ()))


def split(value):
    high = value.astype(BF16)
    return high, (value - high.astype(F32)).astype(BF16)


def contract_kernel(plan, ready, raw, kept, added, closing, pairs, blocks, places, ints, chosen, energies, *refs):
    p_slots, plan, near_slots, silent, inner_only = plan
    ids_at, bases_at, inner_at, rep_at, count_at = places
    slots = sorted(ready + raw)
    near_at, meta_at = ints.shape[0] - 1 - pairs, ints.shape[0] - 1
    refs = list(refs)

    def take(names):
        return {name: refs.pop(0) for name in names}

    dense = take(ready)
    units = take(raw)
    exts = take(slots)
    addends = take(added)
    outs = take(p_slots)
    shown = refs.pop(0) if closing else None
    dense.update(take(kept))
    dense.update(take([u for u in raw if u not in kept]))
    x_hi, x_lo, v_hi, v_lo, diag, near, inv = refs
    rows = pairs * NPNO
    halves = pairs // 2
    inner = ints[meta_at, inner_at].astype(F32)
    for n, u in enumerate(raw):
        for j in range(pairs):
            here = (n * pairs + j) * NBLK
            for d in range(NBLK):
                inv[here + d] = ABSENT
            for a in range(blocks):
                inv[here + ints[a, ints[meta_at, bases_at + u] + j]] = a
    for n, u in enumerate(raw):
        for j in range(pairs):
            for d in range(NBLK):
                at = inv[(n * pairs + j) * NBLK + d]
                block = units[u][j * blocks + (at & (ABSENT - 1))]
                dense[u][pl.ds(j * NPNO, NPNO), pl.ds(d * 128, 128)] = jnp.where(
                    at < ABSENT, block, jnp.zeros((), BF16)
                )
    diag[...] = jnp.zeros(diag.shape, BF16)
    lane = lax.broadcasted_iota(jnp.int32, (1, rows), 1)
    pair_of_lane = (lane // NPNO).astype(F32)
    left = lax.broadcasted_iota(jnp.int32, (NPNO, 128), 1) < NPNO
    if near_slots:
        group = near.shape[0]
        members = lax.broadcasted_iota(jnp.int32, (group, chosen.shape[1]), 0)
        lanes = lax.broadcasted_iota(jnp.int32, (group, rows), 1) // NPNO
        times = jnp.zeros((group, rows), F32)
        for j in range(pairs):
            hits = jnp.where(chosen[near_at + j : near_at + j + 1, :] == members, 1.0, 0.0)
            times = jnp.where(lanes == j, jnp.sum(hits, axis=1, keepdims=True), times)
        near[...] = times
    q_slots = sorted({q for q, _ in plan})
    for n, u in enumerate(q_slots):
        for j in range(pairs):
            tile = exts[u][j // 2, :NPNO, :]
            keep = left if j % 2 == 0 else jnp.logical_not(left)
            diag[n, pl.ds(j * NPNO, NPNO), pl.ds((j // 2) * 128, 128)] = jnp.where(
                keep, tile, jnp.zeros((), BF16)
            )

    row = lax.broadcasted_iota(jnp.int32, (rows, rows), 0) // NPNO
    col = lax.broadcasted_iota(jnp.int32, (rows, rows), 1) // NPNO
    own_block = row == col
    spots = {block: pl.ds(n * rows, rows) for n, block in enumerate(plan)}
    for u, s in plan:
        x = lax.dot_general(dense[u][...], dense[s][...], NT, preferred_element_type=F32)
        x_hi[spots[u, s], :], x_lo[spots[u, s], :] = split(x)
    for u, s in plan:
        here = spots[u, s]
        amps = diag[q_slots.index(u)]
        v = jnp.dot(amps, x_hi[here, :], preferred_element_type=F32)
        v += jnp.dot(amps, x_lo[here, :], preferred_element_type=F32)
        p_id = ints[meta_at, ids_at + s].astype(F32) + pair_of_lane
        tails = [exts[s][h, NPNO:, :].astype(F32) for h in range(halves)]
        p_codes = [jnp.concatenate([t[k : k + 1] for t in tails], axis=1) for k in range(2)]
        strips = []
        for j in range(pairs):
            weight = jnp.zeros((1, rows), F32)
            if (u, s) not in silent:
                q_id = (ints[meta_at, ids_at + u] + j).astype(F32)
                q_tail = exts[u][j // 2, NPNO:, :].astype(F32)
                for k in range(2):
                    at = 2 + 2 * (j % 2) + k
                    q_code = jnp.concatenate([q_tail[at : at + 1]] * halves, axis=1)
                    weight = weight + jnp.where(q_code == p_id, 1.0, 0.0)
                    weight = weight + jnp.where(p_codes[k] == q_id, 1.0, 0.0)
                if (u, s) in inner_only:
                    weight = weight * inner
            if u in near_slots and s == p_slots[0]:
                at = (ints[meta_at, rep_at] ^ near_slots[u]) * pairs + j
                weight = weight + near[pl.ds(at, 1), :]
            strips.append(v[j * NPNO : (j + 1) * NPNO] * weight)
        v_hi[here, :], v_lo[here, :] = split(jnp.concatenate(strips, axis=0))
    for s in p_slots:
        mine = [n for n, block in enumerate(plan) if block[1] == s]
        deep = pl.ds(mine[0] * rows, len(mine) * rows)
        xh, xl, vh, vl = x_hi[deep, :], x_lo[deep, :], v_hi[deep, :], v_lo[deep, :]
        total = lax.dot_general(xh, vh, TN, preferred_element_type=F32)
        total += lax.dot_general(xh, vl, TN, preferred_element_type=F32)
        total += lax.dot_general(xl, vh, TN, preferred_element_type=F32)
        total = jnp.where(own_block, total, 0.0)
        for h in range(halves):
            two = total[h * 128 : (h + 1) * 128, h * 128 : (h + 1) * 128]
            two = two[:NPNO] + two[NPNO:]
            if s in added:
                two = two + addends[s][h]
            if closing:
                even, odd = energies[2 * h : 2 * h + 1, :], energies[2 * h + 1 : 2 * h + 2, :]
                a = lax.broadcasted_iota(jnp.int32, (NPNO, 128), 0)
                b = lax.broadcasted_iota(jnp.int32, (NPNO, 128), 1)
                down = [
                    jnp.sum(jnp.where(a == b, e, 0.0), axis=1, keepdims=True) for e in (even, odd)
                ]
                both = jnp.where(left, even, odd) + jnp.where(left, *down)
                two = two + both * exts[s][h, :NPNO, :].astype(F32)
                live = jnp.where(
                    left, ints[meta_at, count_at + 2 * h], ints[meta_at, count_at + 2 * h + 1]
                )
                seen = jnp.logical_and(a < live, jnp.where(left, b, b - NPNO) < live)
                shown[h] = jnp.where(seen, 1.0, 0.0)
            outs[s][h] = two


def contract(
    dense,
    units,
    exts,
    small,
    places,
    plan,
    kept=(),
    addends=None,
    closing=False,
    near_slots=None,
    silent=(),
    inner_only=(),
):
    ready, raw = sorted(dense), sorted(units)
    slots = sorted(ready + raw)
    kept = sorted(kept)
    p_slots = sorted({p for _, p in plan})
    plan = sorted(plan, key=lambda block: block[1])
    pairs = exts[slots[0]].shape[0] * 2
    addends = addends or {}
    added = sorted(addends)
    blocks = units[raw[0]].shape[0] // pairs if raw else 0
    rows = pairs * NPNO
    deep = rows * len(plan)
    group = lax.axis_size("rep") * pairs
    wide = NBLK * 128
    smem = pl.BlockSpec(memory_space=pltpu.SMEM)
    vmem = pl.BlockSpec(memory_space=pltpu.VMEM)
    plan = (p_slots, plan, near_slots or {}, frozenset(silent), frozenset(inner_only))
    body = functools.partial(
        contract_kernel, plan, ready, raw, kept, added, closing, pairs, blocks, places
    )
    q_count = len({q for q, _ in plan[1]})
    results = pl.pallas_call(
        body,
        out_shape=[jax.ShapeDtypeStruct((pairs // 2, NPNO, 128), F32)] * (len(p_slots) + closing)
        + [jax.ShapeDtypeStruct((rows, wide), BF16)] * len(kept),
        in_specs=[smem, vmem, vmem] + [vmem] * (2 * len(slots) + len(added)),
        out_specs=[vmem] * (len(p_slots) + closing + len(kept)),
        scratch_shapes=[pltpu.VMEM((rows, wide), BF16)] * (len(raw) - len(kept))
        + [pltpu.VMEM((deep, rows), BF16)] * 4
        + [
            pltpu.VMEM((q_count, rows, rows), BF16),
            pltpu.VMEM((group, rows), F32),
            pltpu.SMEM((max(1, len(raw)) * pairs * NBLK,), jnp.int32),
        ],
        cost_estimate=pl.CostEstimate(
            flops=2 * deep * rows * (wide + 5 * rows), bytes_accessed=0, transcendentals=0
        ),
        compiler_params=pltpu.CompilerParams(vmem_limit_bytes=GRANT),
    )(
        *small,
        *[dense[u] for u in ready],
        *[units[u] for u in raw],
        *[exts[u] for u in slots],
        *[addends[s] for s in added],
    )
    sums = dict(zip(p_slots, results))
    if closing:
        sums["shown"] = results[len(p_slots)]
    return sums, dict(zip(kept, results[len(p_slots) + closing :]))


def pack(square):
    pairs = square.shape[0]
    return (
        square.reshape(pairs // 2, 2, NPNO, NPNO).transpose(0, 2, 1, 3).reshape(pairs // 2, NPNO, 128)
    )


def unpack(packed):
    halves = packed.shape[0]
    return packed.reshape(halves, NPNO, 2, NPNO).transpose(0, 2, 1, 3).reshape(2 * halves, NPNO * NPNO)


def residual_of(coeffs, amplitudes, denominators, pno_count, domains, far_owner, far_pair, near_pair):
    pairs, blocks = coeffs.shape[:2]
    occ_count = lax.axis_size("occ")
    rep_count = lax.axis_size("rep")
    occ = lax.axis_index("occ")
    rep = lax.axis_index("rep")
    live_rows = jnp.arange(NPNO, dtype=jnp.int32)[None, :] < pno_count[:, None]
    live_both = live_rows[:, :, None] & live_rows[:, None, :]
    amps = jnp.where(
        live_both, amplitudes.reshape(pairs, NPNO, NPNO), jnp.zeros((), BF16)
    )
    codes = (far_owner * pairs + far_pair + 1).astype(BF16).reshape(pairs // 2, 2, 2)
    ext = jnp.concatenate(
        [
            pack(amps),
            jnp.broadcast_to(
                codes.transpose(0, 2, 1)[..., None], (pairs // 2, 2, 2, NPNO)
            ).reshape(pairs // 2, 2, 128),
            jnp.broadcast_to(codes.reshape(pairs // 2, 4, 1), (pairs // 2, 4, 128)),
            jnp.zeros((pairs // 2, 2, 128), BF16),
        ],
        axis=1,
    )
    own = coeffs.reshape(pairs * blocks, NPNO, 128)
    nobody = jnp.full((), NOBODY, jnp.int32)

    energies = jnp.concatenate([denominators, denominators], axis=1)

    def small_of(ids, bases, inner, rep_now):
        values = [jnp.asarray(v, jnp.int32) for v in (*ids, *bases, inner, rep_now)]
        count = len(ids)
        wide = max(domains.shape[0], 128)

        def fit(rows):
            return jnp.pad(rows, ((0, 0), (0, wide - rows.shape[1])), constant_values=-1)

        scalars = jnp.concatenate([jnp.stack(values), pno_count])[None, :]
        ints = jnp.concatenate([fit(domains.T), fit(near_pair), fit(scalars)], axis=0)
        return (ints, ints, energies), (0, count, 2 * count, 2 * count + 1, 2 * count + 2)

    def pair_base(o, r):
        return (o * rep_count + r) * pairs

    if occ_count == 8 and rep_count == 4:
        layer, side = occ // 2, occ % 2
        inner = (layer == 1) | (layer == 2)
        near_layer = layer ^ 1
        far_end = jnp.where(layer < 2, 3, 0)
        OWN, OUT, MID, SIDE, MID2, SIDE2, CORE, ROW, BOTH = range(9)
        occ_ids = [
            occ,
            near_layer * 2 + side,
            (3 - layer) * 2 + side,
            layer * 2 + 1 - side,
            far_end * 2 + side,
            near_layer * 2 + 1 - side,
        ]
        ids = [o * pairs + 1 for o in occ_ids] + [nobody] * 3
        bases = [pair_base(o, rep) for o in occ_ids]
        bases += [pair_base(occ, rep ^ k) for k in (1, 2, 3)]
        along = [(a, a ^ 2) for a in range(8)]
        middle = [(a, a ^ 6 if 2 <= a < 6 else a) for a in range(8)]
        across = [(a, a ^ 1) for a in range(8)]
        swap_y = [(r, r ^ 2) for r in range(rep_count)]
        swap_core = [(r, r ^ 1) for r in range(rep_count)]

        straight = [(a ^ 4 if 2 <= a < 6 else a ^ 2, a) for a in range(8)]
        oblique = [(a ^ 3, a) for a in range(8)]
        units, exts = {OWN: own}, {OWN: ext}
        for slot, source, axis, perm in (
            (OUT, OWN, "occ", along),
            (MID, OWN, "occ", middle),
            (SIDE, OWN, "occ", across),
            (ROW, OWN, "rep", swap_y),
            (CORE, OWN, "rep", swap_core),
            (MID2, OUT, "occ", middle),
            (SIDE2, OUT, "occ", across),
            (BOTH, ROW, "rep", swap_core),
        ):
            units[slot] = lax.ppermute(units[source], axis, perm)
            if slot in (MID2, SIDE2):
                source, perm = OWN, straight if slot == MID2 else oblique
            exts[slot] = lax.ppermute(exts[source], axis, perm)
        small, places = small_of(ids, bases, inner, rep)
        dense = {}

        def run(plan, keep=(), **kwargs):
            slots = {slot for block in plan for slot in block}
            result, made = contract(
                {slot: dense[slot] for slot in slots if slot in dense},
                {slot: units[slot] for slot in slots if slot not in dense},
                {slot: exts[slot] for slot in slots},
                small,
                places,
                plan,
                kept=keep,
                **kwargs,
            )
            dense.update(made)
            return result

        first = run(
            (
                (OWN, OWN),
                (CORE, OWN),
                (OUT, OWN),
                (MID, OWN),
                (SIDE, OWN),
                (MID, OUT),
                (SIDE, OUT),
                (ROW, OWN),
                (MID, SIDE),
            ),
            keep=(OWN, OUT, MID, SIDE),
            near_slots={OWN: 0, CORE: 1, ROW: 2},
            silent=((CORE, OWN), (ROW, OWN)),
            inner_only=((MID, OWN), (MID, OUT), (SIDE, OUT), (MID, SIDE)),
        )
        crossing = [(MID, SIDE2), (MID2, SIDE), (MID2, SIDE2), (MID2, OUT)]
        tail = run(
            crossing,
            keep=(MID2, SIDE2),
            addends={OUT: first[OUT], SIDE: first[SIDE]},
            inner_only=crossing,
        )
        returned = [
            lax.ppermute(tail[SIDE], "occ", across),
            lax.ppermute(tail[SIDE2], "occ", oblique),
            lax.ppermute(tail[OUT], "occ", along),
        ]
        close = run(
            ((MID2, OWN), (SIDE2, OWN), (BOTH, OWN)),
            addends={OWN: first[OWN]},
            closing=True,
            near_slots={BOTH: 3},
            silent=((BOTH, OWN),),
            inner_only=((MID2, OWN), (SIDE2, OWN)),
        )
        gain = close[OWN] + sum(returned)
        mask = close["shown"]
    else:
        group_units = lax.all_gather(own, "rep", axis=0)
        group_exts = lax.all_gather(ext, "rep", axis=0)
        line_units = lax.all_gather(own, "occ", axis=0)
        line_exts = lax.all_gather(ext, "occ", axis=0)

        def add_near(total, k):
            r = rep ^ k
            small, places = small_of(
                [nobody, nobody], [pair_base(occ, rep), pair_base(occ, r)], 1, r
            )
            part, _ = contract(
                {},
                {0: own, 1: group_units[r]},
                {0: ext, 1: group_exts[r]},
                small,
                places,
                ((1, 0),),
                near_slots={1: 0},
                silent=((1, 0),),
            )
            return total + part[0], None

        def add_far(total, o):
            small, places = small_of(
                [occ * pairs + 1, o * pairs + 1], [pair_base(occ, rep), pair_base(o, rep)], 1, rep
            )
            part, _ = contract(
                {},
                {0: own, 1: line_units[o]},
                {0: ext, 1: line_exts[o]},
                small,
                places,
                ((1, 0),),
            )
            return total + part[0], None

        gain = pack((denominators[:, :, None] + denominators[:, None, :]) * amps.astype(F32))
        mask = pack(live_both.astype(F32))
        gain, _ = lax.scan(add_near, gain, jnp.arange(rep_count, dtype=jnp.int32))
        gain, _ = lax.scan(add_far, gain, jnp.arange(occ_count, dtype=jnp.int32))
    return unpack(jnp.where(mask > 0, gain, 0.0))


def solution(mesh):
    in_specs = (
        P(("occ", "rep"), None, None, None),
        P(("occ", "rep"), None),
        P(("occ", "rep"), None),
        P(("occ", "rep")),
        P(),
        P(("occ", "rep"), None),
        P(("occ", "rep"), None),
        P(("occ", "rep"), None),
    )
    out_specs = P(("occ", "rep"), None)
    return jax.shard_map(
        residual_of, mesh=mesh, in_specs=in_specs, out_specs=out_specs, check_vma=False
    )
```

```python
import functools

import jax
import jax.numpy as jnp
from jax import lax
from jax.experimental import pallas as pl
from jax.experimental.pallas import tpu as pltpu
from jax.sharding import PartitionSpec as P


NPNO = 64
NBLK = 32
ABSENT = 1 << 10
GRANT = 16 << 20
NOBODY = -(1 << 16)
F32 = jnp.float32
BF16 = jnp.bfloat16
NT = (((1,), (1,)), ((), ()))
TN = (((0,), (0,)), ((), ()))


def split(value):
    high = value.astype(BF16)
    return high, (value - high.astype(F32)).astype(BF16)


def contract_kernel(plan, ready, raw, kept, added, closing, pairs, blocks, places, ints, chosen, energies, *refs):
    p_slots, plan, near_slots, silent, inner_only = plan
    ids_at, bases_at, inner_at, rep_at, count_at = places
    slots = sorted(ready + raw)
    near_at, meta_at = ints.shape[0] - 1 - pairs, ints.shape[0] - 1
    refs = list(refs)

    def take(names):
        return {name: refs.pop(0) for name in names}

    dense = take(ready)
    units = take(raw)
    exts = take(slots)
    addends = take(added)
    outs = take(p_slots)
    shown = refs.pop(0) if closing else None
    dense.update(take(kept))
    dense.update(take([u for u in raw if u not in kept]))
    x_hi, x_lo, v_hi, v_lo, diag, near, inv = refs
    rows = pairs * NPNO
    halves = pairs // 2
    inner = ints[meta_at, inner_at].astype(F32)
    for n, u in enumerate(raw):
        for j in range(pairs):
            here = (n * pairs + j) * NBLK
            for d in range(NBLK):
                inv[here + d] = ABSENT
            for a in range(blocks):
                inv[here + ints[a, ints[meta_at, bases_at + u] + j]] = a
    for n, u in enumerate(raw):
        for j in range(pairs):
            for d in range(NBLK):
                at = inv[(n * pairs + j) * NBLK + d]
                block = units[u][j * blocks + (at & (ABSENT - 1))]
                dense[u][pl.ds(j * NPNO, NPNO), pl.ds(d * 128, 128)] = jnp.where(
                    at < ABSENT, block, jnp.zeros((), BF16)
                )
    diag[...] = jnp.zeros(diag.shape, BF16)
    lane = lax.broadcasted_iota(jnp.int32, (1, rows), 1)
    pair_of_lane = (lane // NPNO).astype(F32)
    left = lax.broadcasted_iota(jnp.int32, (NPNO, 128), 1) < NPNO
    if near_slots:
        group = near.shape[0]
        members = lax.broadcasted_iota(jnp.int32, (group, chosen.shape[1]), 0)
        lanes = lax.broadcasted_iota(jnp.int32, (group, rows), 1) // NPNO
        times = jnp.zeros((group, rows), F32)
        for j in range(pairs):
            hits = jnp.where(chosen[near_at + j : near_at + j + 1, :] == members, 1.0, 0.0)
            times = jnp.where(lanes == j, jnp.sum(hits, axis=1, keepdims=True), times)
        near[...] = times
    q_slots = sorted({q for q, _ in plan})
    for n, u in enumerate(q_slots):
        for j in range(pairs):
            tile = exts[u][j // 2, :NPNO, :]
            keep = left if j % 2 == 0 else jnp.logical_not(left)
            diag[n, pl.ds(j * NPNO, NPNO), pl.ds((j // 2) * 128, 128)] = jnp.where(
                keep, tile, jnp.zeros((), BF16)
            )

    row = lax.broadcasted_iota(jnp.int32, (rows, rows), 0) // NPNO
    col = lax.broadcasted_iota(jnp.int32, (rows, rows), 1) // NPNO
    own_block = row == col
    spots = {block: pl.ds(n * rows, rows) for n, block in enumerate(plan)}
    for u, s in plan:
        x = lax.dot_general(dense[u][...], dense[s][...], NT, preferred_element_type=F32)
        x_hi[spots[u, s], :], x_lo[spots[u, s], :] = split(x)
    for u, s in plan:
        here = spots[u, s]
        amps = diag[q_slots.index(u)]
        v = jnp.dot(amps, x_hi[here, :], preferred_element_type=F32)
        v += jnp.dot(amps, x_lo[here, :], preferred_element_type=F32)
        p_id = ints[meta_at, ids_at + s].astype(F32) + pair_of_lane
        tails = [exts[s][h, NPNO:, :].astype(F32) for h in range(halves)]
        p_codes = [jnp.concatenate([t[k : k + 1] for t in tails], axis=1) for k in range(2)]
        strips = []
        for j in range(pairs):
            weight = jnp.zeros((1, rows), F32)
            if (u, s) not in silent:
                q_id = (ints[meta_at, ids_at + u] + j).astype(F32)
                q_tail = exts[u][j // 2, NPNO:, :].astype(F32)
                for k in range(2):
                    at = 2 + 2 * (j % 2) + k
                    q_code = jnp.concatenate([q_tail[at : at + 1]] * halves, axis=1)
                    weight = weight + jnp.where(q_code == p_id, 1.0, 0.0)
                    weight = weight + jnp.where(p_codes[k] == q_id, 1.0, 0.0)
                if (u, s) in inner_only:
                    weight = weight * inner
            if u in near_slots and s == p_slots[0]:
                at = (ints[meta_at, rep_at] ^ near_slots[u]) * pairs + j
                weight = weight + near[pl.ds(at, 1), :]
            strips.append(v[j * NPNO : (j + 1) * NPNO] * weight)
        v_hi[here, :], v_lo[here, :] = split(jnp.concatenate(strips, axis=0))
    for s in p_slots:
        mine = [n for n, block in enumerate(plan) if block[1] == s]
        deep = pl.ds(mine[0] * rows, len(mine) * rows)
        xh, xl, vh, vl = x_hi[deep, :], x_lo[deep, :], v_hi[deep, :], v_lo[deep, :]
        total = lax.dot_general(xh, vh, TN, preferred_element_type=F32)
        total += lax.dot_general(xh, vl, TN, preferred_element_type=F32)
        total += lax.dot_general(xl, vh, TN, preferred_element_type=F32)
        total = jnp.where(own_block, total, 0.0)
        for h in range(halves):
            two = total[h * 128 : (h + 1) * 128, h * 128 : (h + 1) * 128]
            two = two[:NPNO] + two[NPNO:]
            if s in added:
                two = two + addends[s][h]
            if closing:
                even, odd = energies[2 * h : 2 * h + 1, :], energies[2 * h + 1 : 2 * h + 2, :]
                a = lax.broadcasted_iota(jnp.int32, (NPNO, 128), 0)
                b = lax.broadcasted_iota(jnp.int32, (NPNO, 128), 1)
                down = [
                    jnp.sum(jnp.where(a == b, e, 0.0), axis=1, keepdims=True) for e in (even, odd)
                ]
                both = jnp.where(left, even, odd) + jnp.where(left, *down)
                two = two + both * exts[s][h, :NPNO, :].astype(F32)
                live = jnp.where(
                    left, ints[meta_at, count_at + 2 * h], ints[meta_at, count_at + 2 * h + 1]
                )
                seen = jnp.logical_and(a < live, jnp.where(left, b, b - NPNO) < live)
                shown[h] = jnp.where(seen, 1.0, 0.0)
            outs[s][h] = two


def contract(
    dense,
    units,
    exts,
    small,
    places,
    plan,
    kept=(),
    addends=None,
    closing=False,
    near_slots=None,
    silent=(),
    inner_only=(),
):
    ready, raw = sorted(dense), sorted(units)
    slots = sorted(ready + raw)
    kept = sorted(kept)
    p_slots = sorted({p for _, p in plan})
    plan = sorted(plan, key=lambda block: block[1])
    pairs = exts[slots[0]].shape[0] * 2
    addends = addends or {}
    added = sorted(addends)
    blocks = units[raw[0]].shape[0] // pairs if raw else 0
    rows = pairs * NPNO
    deep = rows * len(plan)
    group = lax.axis_size("rep") * pairs
    wide = NBLK * 128
    smem = pl.BlockSpec(memory_space=pltpu.SMEM)
    vmem = pl.BlockSpec(memory_space=pltpu.VMEM)
    plan = (p_slots, plan, near_slots or {}, frozenset(silent), frozenset(inner_only))
    body = functools.partial(
        contract_kernel, plan, ready, raw, kept, added, closing, pairs, blocks, places
    )
    q_count = len({q for q, _ in plan[1]})
    results = pl.pallas_call(
        body,
        out_shape=[jax.ShapeDtypeStruct((pairs // 2, NPNO, 128), F32)] * (len(p_slots) + closing)
        + [jax.ShapeDtypeStruct((rows, wide), BF16)] * len(kept),
        in_specs=[smem, vmem, vmem] + [vmem] * (2 * len(slots) + len(added)),
        out_specs=[vmem] * (len(p_slots) + closing + len(kept)),
        scratch_shapes=[pltpu.VMEM((rows, wide), BF16)] * (len(raw) - len(kept))
        + [pltpu.VMEM((deep, rows), BF16)] * 4
        + [
            pltpu.VMEM((q_count, rows, rows), BF16),
            pltpu.VMEM((group, rows), F32),
            pltpu.SMEM((max(1, len(raw)) * pairs * NBLK,), jnp.int32),
        ],
        cost_estimate=pl.CostEstimate(
            flops=2 * deep * rows * (wide + 5 * rows), bytes_accessed=0, transcendentals=0
        ),
        compiler_params=pltpu.CompilerParams(vmem_limit_bytes=GRANT),
    )(
        *small,
        *[dense[u] for u in ready],
        *[units[u] for u in raw],
        *[exts[u] for u in slots],
        *[addends[s] for s in added],
    )
    sums = dict(zip(p_slots, results))
    if closing:
        sums["shown"] = results[len(p_slots)]
    return sums, dict(zip(kept, results[len(p_slots) + closing :]))


def pack(square):
    pairs = square.shape[0]
    return (
        square.reshape(pairs // 2, 2, NPNO, NPNO).transpose(0, 2, 1, 3).reshape(pairs // 2, NPNO, 128)
    )


def unpack(packed):
    halves = packed.shape[0]
    return packed.reshape(halves, NPNO, 2, NPNO).transpose(0, 2, 1, 3).reshape(2 * halves, NPNO * NPNO)


def residual_of(coeffs, amplitudes, denominators, pno_count, domains, far_owner, far_pair, near_pair):
    pairs, blocks = coeffs.shape[:2]
    occ_count = lax.axis_size("occ")
    rep_count = lax.axis_size("rep")
    occ = lax.axis_index("occ")
    rep = lax.axis_index("rep")
    live_rows = jnp.arange(NPNO, dtype=jnp.int32)[None, :] < pno_count[:, None]
    live_both = live_rows[:, :, None] & live_rows[:, None, :]
    amps = jnp.where(
        live_both, amplitudes.reshape(pairs, NPNO, NPNO), jnp.zeros((), BF16)
    )
    codes = (far_owner * pairs + far_pair + 1).astype(BF16).reshape(pairs // 2, 2, 2)
    ext = jnp.concatenate(
        [
            pack(amps),
            jnp.broadcast_to(
                codes.transpose(0, 2, 1)[..., None], (pairs // 2, 2, 2, NPNO)
            ).reshape(pairs // 2, 2, 128),
            jnp.broadcast_to(codes.reshape(pairs // 2, 4, 1), (pairs // 2, 4, 128)),
            jnp.zeros((pairs // 2, 2, 128), BF16),
        ],
        axis=1,
    )
    own = coeffs.reshape(pairs * blocks, NPNO, 128)
    nobody = jnp.full((), NOBODY, jnp.int32)

    energies = jnp.concatenate([denominators, denominators], axis=1)

    def small_of(ids, bases, inner, rep_now):
        values = [jnp.asarray(v, jnp.int32) for v in (*ids, *bases, inner, rep_now)]
        count = len(ids)
        wide = max(domains.shape[0], 128)

        def fit(rows):
            return jnp.pad(rows, ((0, 0), (0, wide - rows.shape[1])), constant_values=-1)

        scalars = jnp.concatenate([jnp.stack(values), pno_count])[None, :]
        ints = jnp.concatenate([fit(domains.T), fit(near_pair), fit(scalars)], axis=0)
        return (ints, ints, energies), (0, count, 2 * count, 2 * count + 1, 2 * count + 2)

    def pair_base(o, r):
        return (o * rep_count + r) * pairs

    if occ_count == 8 and rep_count == 4:
        layer, side = occ // 2, occ % 2
        inner = (layer == 1) | (layer == 2)
        near_layer = layer ^ 1
        far_end = jnp.where(layer < 2, 3, 0)
        OWN, OUT, MID, SIDE, MID2, SIDE2, CORE, ROW, BOTH = range(9)
        occ_ids = [
            occ,
            near_layer * 2 + side,
            (3 - layer) * 2 + side,
            layer * 2 + 1 - side,
            far_end * 2 + side,
            near_layer * 2 + 1 - side,
        ]
        ids = [o * pairs + 1 for o in occ_ids] + [nobody] * 3
        bases = [pair_base(o, rep) for o in occ_ids]
        bases += [pair_base(occ, rep ^ k) for k in (1, 2, 3)]
        along = [(a, a ^ 2) for a in range(8)]
        middle = [(a, a ^ 6 if 2 <= a < 6 else a) for a in range(8)]
        across = [(a, a ^ 1) for a in range(8)]
        swap_y = [(r, r ^ 2) for r in range(rep_count)]
        swap_core = [(r, r ^ 1) for r in range(rep_count)]

        straight = [(a ^ 4 if 2 <= a < 6 else a ^ 2, a) for a in range(8)]
        oblique = [(a ^ 3, a) for a in range(8)]
        units, exts = {OWN: own}, {OWN: ext}
        for slot, source, axis, perm in (
            (OUT, OWN, "occ", along),
            (MID, OWN, "occ", middle),
            (SIDE, OWN, "occ", across),
            (ROW, OWN, "rep", swap_y),
            (CORE, OWN, "rep", swap_core),
            (MID2, OUT, "occ", middle),
            (SIDE2, OUT, "occ", across),
            (BOTH, ROW, "rep", swap_core),
        ):
            units[slot] = lax.ppermute(units[source], axis, perm)
            if slot in (MID2, SIDE2):
                source, perm = OWN, straight if slot == MID2 else oblique
            exts[slot] = lax.ppermute(exts[source], axis, perm)
        small, places = small_of(ids, bases, inner, rep)
        dense = {}

        def run(plan, keep=(), **kwargs):
            slots = {slot for block in plan for slot in block}
            result, made = contract(
                {slot: dense[slot] for slot in slots if slot in dense},
                {slot: units[slot] for slot in slots if slot not in dense},
                {slot: exts[slot] for slot in slots},
                small,
                places,
                plan,
                kept=keep,
                **kwargs,
            )
            dense.update(made)
            return result

        first = run(
            (
                (OWN, OWN),
                (CORE, OWN),
                (OUT, OWN),
                (MID, OWN),
                (SIDE, OWN),
                (MID, OUT),
                (SIDE, OUT),
                (ROW, OWN),
                (MID, SIDE),
            ),
            keep=(OWN, OUT, MID, SIDE),
            near_slots={OWN: 0, CORE: 1, ROW: 2},
            silent=((CORE, OWN), (ROW, OWN)),
            inner_only=((MID, OWN), (MID, OUT), (SIDE, OUT), (MID, SIDE)),
        )
        apart = run(
            ((BOTH, OWN),), addends={OWN: first[OWN]}, near_slots={BOTH: 3}, silent=((BOTH, OWN),)
        )
        first[OUT], apart[OWN] = lax.optimization_barrier((first[OUT], apart[OWN]))
        crossing = [(MID, SIDE2), (MID2, SIDE), (MID2, SIDE2), (MID2, OUT)]
        tail = run(
            crossing,
            keep=(MID2, SIDE2),
            addends={OUT: first[OUT], SIDE: first[SIDE]},
            inner_only=crossing,
        )
        returned = [
            lax.ppermute(tail[SIDE], "occ", across),
            lax.ppermute(tail[SIDE2], "occ", oblique),
            lax.ppermute(tail[OUT], "occ", along),
        ]
        close = run(
            ((MID2, OWN), (SIDE2, OWN)),
            addends={OWN: apart[OWN]},
            closing=True,
            inner_only=((MID2, OWN), (SIDE2, OWN)),
        )
        gain = close[OWN] + sum(returned)
        mask = close["shown"]
    else:
        group_units = lax.all_gather(own, "rep", axis=0)
        group_exts = lax.all_gather(ext, "rep", axis=0)
        line_units = lax.all_gather(own, "occ", axis=0)
        line_exts = lax.all_gather(ext, "occ", axis=0)

        def add_near(total, k):
            r = rep ^ k
            small, places = small_of(
                [nobody, nobody], [pair_base(occ, rep), pair_base(occ, r)], 1, r
            )
            part, _ = contract(
                {},
                {0: own, 1: group_units[r]},
                {0: ext, 1: group_exts[r]},
                small,
                places,
                ((1, 0),),
                near_slots={1: 0},
                silent=((1, 0),),
            )
            return total + part[0], None

        def add_far(total, o):
            small, places = small_of(
                [occ * pairs + 1, o * pairs + 1], [pair_base(occ, rep), pair_base(o, rep)], 1, rep
            )
            part, _ = contract(
                {},
                {0: own, 1: line_units[o]},
                {0: ext, 1: line_exts[o]},
                small,
                places,
                ((1, 0),),
            )
            return total + part[0], None

        gain = pack((denominators[:, :, None] + denominators[:, None, :]) * amps.astype(F32))
        mask = pack(live_both.astype(F32))
        gain, _ = lax.scan(add_near, gain, jnp.arange(rep_count, dtype=jnp.int32))
        gain, _ = lax.scan(add_far, gain, jnp.arange(occ_count, dtype=jnp.int32))
    return unpack(jnp.where(mask > 0, gain, 0.0))


def solution(mesh):
    in_specs = (
        P(("occ", "rep"), None, None, None),
        P(("occ", "rep"), None),
        P(("occ", "rep"), None),
        P(("occ", "rep")),
        P(),
        P(("occ", "rep"), None),
        P(("occ", "rep"), None),
        P(("occ", "rep"), None),
    )
    out_specs = P(("occ", "rep"), None)
    return jax.shard_map(
        residual_of, mesh=mesh, in_specs=in_specs, out_specs=out_specs, check_vma=False
    )
```
